128 devices in a mesh: sys: 1, zdom: 2 (over core), ydom: 64 (over z, y, x).
Axes of the slice: x: 4, y: 4, z: 4, core: 2. Of those that a mesh axis runs over, the one named last changes fastest.
Arguments:
- charge: float32 [2097152], P(('sys', 'ydom', 'zdom'))
- real_mask: int32 [2097152], P(('sys', 'ydom', 'zdom'))
- grid_idx: int32 [2097152, 3], P(('sys', 'ydom', 'zdom'))
- spline_w: float32 [2097152, 3, 4], P(('sys', 'ydom', 'zdom'))
- influence: float32 [384, 384, 384], P(('sys', 'ydom'), 'zdom')
Outputs:
- output 1: float32 [384, 384, 384], P(('sys', 'ydom'), 'zdom')
- output 2: float32 [1], P('sys')
All inputs are finite; a program needn't handle non-finite values.
Results may differ from the reference program's by a relative error of at most 0.001.
Values are sent between devices in bfloat16 or wider.
A program may use at most 1 GiB of HBM per device.

```python
import jax
import jax.numpy as jnp
from jax import lax

GRID_SIDE = 384
PER_DEV = 16384
Y_DEVS = 64
Z_DEVS = 2


def bspline_weights(frac_part):
    frac_sq = frac_part * frac_part
    frac_cube = frac_sq * frac_part
    w_zero = (1.0 - frac_part) * (1.0 - frac_part) * (1.0 - frac_part) / 6.0
    w_one = (3.0 * frac_cube - 6.0 * frac_sq + 4.0) / 6.0
    w_two = (-3.0 * frac_cube + 3.0 * frac_sq + 3.0 * frac_part + 1.0) / 6.0
    w_three = frac_cube / 6.0
    return jnp.stack([w_zero, w_one, w_two, w_three], axis=-1)


def edge_index(key, count, length):
    key_near, key_edge, key_any = jax.random.split(key, 3)
    near_edge = jax.random.randint(key_near, (count,), 0, 2)
    at_edge = length - 3 + jax.random.randint(key_edge, (count,), 0, 3)
    anywhere = jax.random.randint(key_any, (count,), 0, length)
    return jnp.where(near_edge == 1, at_edge, anywhere)


def setup_inputs(seed: int = 0, part: int = 0) -> dict:
    dev_count = Y_DEVS * Z_DEVS
    slot_count = dev_count * PER_DEV
    len_y = GRID_SIDE // Y_DEVS
    len_z = GRID_SIDE // Z_DEVS
    sub_keys = jax.random.split(jax.random.fold_in(jax.random.key(seed), part), 8)
    real_count = jax.random.randint(sub_keys[0], (dev_count, 1), PER_DEV // 8, PER_DEV + 1)
    slot_rank = jax.random.randint(sub_keys[1], (dev_count, PER_DEV), 0, PER_DEV)
    real_mask = (slot_rank < real_count).astype(jnp.int32).reshape(slot_count)
    x_idx = jax.random.randint(sub_keys[2], (slot_count,), 0, GRID_SIDE)
    y_idx = edge_index(sub_keys[3], slot_count, len_y)
    z_idx = edge_index(sub_keys[4], slot_count, len_z)
    grid_idx = jnp.stack([x_idx, y_idx, z_idx], axis=1).astype(jnp.int32)
    charge = jax.random.normal(sub_keys[5], (slot_count,), jnp.float32)
    frac_part = jax.random.uniform(sub_keys[6], (slot_count, 3), jnp.float32)
    spline_w = bspline_weights(frac_part).astype(jnp.float32)
    influence = jax.random.uniform(sub_keys[7], (GRID_SIDE, GRID_SIDE, GRID_SIDE), jnp.float32, 0.5, 1.5) * (20.0 / slot_count)
    return {'charge': charge, 'real_mask': real_mask, 'grid_idx': grid_idx, 'spline_w': spline_w, 'influence': influence}


def reference(charge, real_mask, grid_idx, spline_w, influence):
    slot_count = Y_DEVS * Z_DEVS * PER_DEV
    len_y = GRID_SIDE // Y_DEVS
    len_z = GRID_SIDE // Z_DEVS
    device = jnp.arange(slot_count) // PER_DEV
    base_x = grid_idx[:, 0]
    base_y = grid_idx[:, 1] + (device // Z_DEVS) * len_y
    base_z = grid_idx[:, 2] + (device % Z_DEVS) * len_z
    weight = charge * real_mask.astype(charge.dtype)

    def add_tap(flat_grid, tap_id):
        off_x = tap_id // 16
        off_y = (tap_id // 4) % 4
        off_z = tap_id % 4
        pos_x = (base_x + off_x) % GRID_SIDE
        pos_y = (base_y + off_y) % GRID_SIDE
        pos_z = (base_z + off_z) % GRID_SIDE
        tap_value = weight * spline_w[:, 0, off_x] * spline_w[:, 1, off_y] * spline_w[:, 2, off_z]
        flat_idx = (pos_x * GRID_SIDE + pos_y) * GRID_SIDE + pos_z
        return flat_grid.at[flat_idx].add(tap_value), None

    flat_grid = lax.scan(add_tap, jnp.zeros((GRID_SIDE * GRID_SIDE * GRID_SIDE,), charge.dtype), jnp.arange(64))[0]
    charge_grid = flat_grid.reshape(GRID_SIDE, GRID_SIDE, GRID_SIDE)
    spectrum = jnp.fft.fftn(charge_grid)
    mode_energy = 0.5 * influence * (spectrum.real * spectrum.real + spectrum.imag * spectrum.imag)
    energy = jnp.sum(mode_energy) / (GRID_SIDE * GRID_SIDE * GRID_SIDE)
    return mode_energy, jnp.reshape(energy, (1,))
```

```python
import functools
import jax
import jax.numpy as jnp
import numpy as np
from jax import lax
from jax.experimental import pallas as pl
from jax.experimental.pallas import tpu as pltpu
from jax.sharding import PartitionSpec as P

G = 384
TAPS = 4
NY = 64
LEN_Y = 6
LEN_Z = 192
EXT_Y = 9
CHUNK = 512
LANES = 128
TILES = 14
COLS = TILES * LANES
ROWS = 12
BLOCK = ROWS * TILES
BF = jnp.bfloat16
F32 = jnp.float32

LOW_TILE = 1
HIGH_TILE = 10


def split_np(table):
    high = table.astype(np.float32).astype(jnp.bfloat16)
    low = (table - high.astype(np.float64)).astype(np.float32).astype(jnp.bfloat16)
    return high, low


def twiddles():
    phase = (np.arange(G)[:, None] * np.arange(G)[None, :]) % G
    angle = phase * (2.0 * np.pi / G)
    cos_part, sine_part = np.cos(angle), np.sin(angle)
    freq = (6 * np.arange(NY)[None, :] + np.arange(6)[:, None]).reshape(-1)
    x_rows = np.concatenate([cos_part[freq], -sine_part[freq]], axis=0)
    both = np.concatenate([cos_part, sine_part], axis=1)
    return split_np(x_rows) + split_np(both)


def split(value):
    high = value.astype(BF)
    return high, (value - high.astype(F32)).astype(BF)


def dot(a, b):
    return lax.dot_general(a, b, (((1,), (0,)), ((), ())), preferred_element_type=F32)


def dot_nt(a, b):
    return lax.dot_general(a, b, (((1,), (1,)), ((), ())), preferred_element_type=F32)


def row_iota(first, rows):
    return lax.broadcasted_iota(jnp.int32, (rows, CHUNK), 0) + first


def pick(rows, positions, weights):
    line = jnp.where(rows == positions[3], weights[3], 0.0)
    for s in (2, 1, 0):
        line = jnp.where(rows == positions[s], weights[s], line)
    return line


def spread_kernel(w_ref, idx_ref, q_ref, m_ref, fh_ref, fl_ref, msg_ref, acc_ref, lz_ref, qh_ref, ql_ref, *bufs):
    slots = q_ref.shape[1]

    def build(step, ah, al, bh, bl):
        span = pl.ds(pl.multiple_of(step * CHUNK, CHUNK), CHUNK)
        charge = q_ref[:, span] * m_ref[:, span].astype(F32)

        def rows16(value):
            return jnp.broadcast_to(value, (16, CHUNK))

        def taps(dim, scale, modulus):
            base = idx_ref[dim : dim + 1, span]
            positions, weights = [], []
            for s in range(TAPS):
                position = base + s
                if modulus is not None:
                    position = jnp.where(position >= modulus, position - modulus, position)
                weight = w_ref[dim, s : s + 1, span]
                positions.append(rows16(position))
                weights.append(rows16(weight if scale is None else weight * scale))
            return positions, weights

        pos_x, wgt_x = taps(0, charge, G)
        for g in range(G // 16):
            high, low = split(pick(row_iota(16 * g, 16), pos_x, wgt_x))
            ah[16 * g : 16 * g + 16, :] = high
            al[16 * g : 16 * g + 16, :] = low
        pos_z, wgt_z = taps(2, None, None)
        for g in range(LEN_Z // 16):
            lz_ref[16 * g : 16 * g + 16, :] = pick(row_iota(16 * g, 16), pos_z, wgt_z)
        pos_y, wgt_y = taps(1, None, None)
        for g in range(4):
            rows = row_iota(16 * g, 16)
            value = pick(lax.shift_right_logical(rows, 2), pos_y, wgt_y) * pick(
                LEN_Z + lax.bitwise_and(rows, 3), pos_z, wgt_z
            )
            high, low = split(value)
            bh[64 + 16 * g : 80 + 16 * g, :] = high
            bl[64 + 16 * g : 80 + 16 * g, :] = low
        for y in range(EXT_Y):
            line = pick(jnp.full((16, CHUNK), y, jnp.int32), pos_y, wgt_y)
            for g in range(LEN_Z // 16):
                if g < 8:
                    first = LANES * (LOW_TILE + y) + 16 * g
                elif y == 8:
                    first = 16 * (g - 8)
                else:
                    first = LANES * HIGH_TILE + 64 * y + 16 * (g - 8)
                high, low = split(lz_ref[16 * g : 16 * g + 16, :] * line)
                bh[first : first + 16, :] = high
                bl[first : first + 16, :] = low

    def accumulate(ah, al, bh, bl):
        for t in range(TILES // 2):
            cols = slice(256 * t, 256 * t + 256)
            part = dot_nt(ah[...], bh[cols, :]) + dot_nt(al[...], bh[cols, :]) + dot_nt(ah[...], bl[cols, :])
            acc_ref[:, cols] += part

    first, second = bufs[:4], bufs[4:]
    acc_ref[...] = jnp.zeros_like(acc_ref)
    build(0, *first)
    chunks = slots // CHUNK

    def body(pair, carry):
        accumulate(*first)
        build(2 * pair + 1, *second)
        accumulate(*second)
        build(jnp.minimum(2 * pair + 2, chunks - 1), *first)
        return carry

    lax.fori_loop(0, chunks // 2, body, 0)

    for t in range(TILES // 2):
        cols = slice(256 * t, 256 * t + 256)
        high, low = split(acc_ref[:, cols])
        qh_ref[:, cols] = high
        ql_ref[:, cols] = low
    for t in range(TILES // 2):
        cols = slice(256 * t, 256 * t + 256)
        part = dot(fh_ref[...], qh_ref[:, cols]) + dot(fl_ref[...], qh_ref[:, cols]) + dot(fh_ref[...], ql_ref[:, cols])
        for half in range(2):
            for r in range(ROWS):
                msg_ref[pl.ds((2 * t + half) * ROWS + r, NY, stride=BLOCK), :] = part[
                    NY * r : NY * r + NY, LANES * half : LANES * half + LANES
                ]


def spread(w, idx, charge, mask, fh, fl):
    return pl.pallas_call(
        spread_kernel,
        out_shape=jax.ShapeDtypeStruct((NY * BLOCK, LANES), F32),
        in_specs=[pl.BlockSpec(memory_space=pltpu.VMEM)] * 6,
        out_specs=pl.BlockSpec(memory_space=pltpu.VMEM),
        scratch_shapes=[
            pltpu.VMEM((G, COLS), F32),
            pltpu.VMEM((LEN_Z, CHUNK), F32),
            pltpu.VMEM((G, COLS), BF),
            pltpu.VMEM((G, COLS), BF),
        ]
        + [
            pltpu.VMEM((G, CHUNK), BF),
            pltpu.VMEM((G, CHUNK), BF),
            pltpu.VMEM((COLS, CHUNK), BF),
            pltpu.VMEM((COLS, CHUNK), BF),
        ]
        * 2,
        compiler_params=pltpu.CompilerParams(vmem_limit_bytes=60 * 1024 * 1024),
        name="spread",
    )(w, idx, charge, mask, fh, fl)


def y_kernel(recv_ref, ghost_ref, ch_ref, cl_ref, out_ref, x_ref, rh_ref, rl_ref):
    lane = lax.broadcasted_iota(jnp.int32, (NY, LANES), 1)

    def tile(t, row):
        return recv_ref[pl.ds(t * ROWS + row, NY, stride=BLOCK), :]

    def before(value):
        return pltpu.roll(value, 1, 0)

    def half_turn(value):
        return pltpu.roll(value, 64, 1)

    for pair in range(3):
        for part in range(2):
            high_tiles = []
            for odd in range(2):
                row = 6 * part + 2 * pair + odd
                edge = tile(0, row)
                ghost = ghost_ref[pl.ds(row, NY, stride=16), :]

                def low(y):
                    moved = pltpu.roll(ghost, LANES - 64 - 4 * y, 1)
                    return tile(LOW_TILE + y, row) + jnp.where(lane < 3, moved, 0.0)

                for y in range(LEN_Y):
                    value = low(y)
                    if y < 3:
                        value = value + before(low(y + 6))
                    x_ref[pl.ds(G * odd + y, NY, stride=LEN_Y), :] = value
                tiles = [tile(HIGH_TILE + k, row) for k in range(3)]
                tiles[0] = tiles[0] + before(tile(HIGH_TILE + 3, row))
                tiles[1] = tiles[1] + jnp.where(lane < 64, before(edge), 0.0)
                high_tiles.append(tiles)
            for k in range(3):
                even, odd = high_tiles[0][k], high_tiles[1][k]
                x_ref[pl.ds(2 * G + 2 * k, NY, stride=LEN_Y), :] = jnp.where(lane < 64, even, half_turn(odd))
                x_ref[pl.ds(2 * G + 2 * k + 1, NY, stride=LEN_Y), :] = jnp.where(lane < 64, half_turn(even), odd)
            for k in range(3):
                high, low_part = split(x_ref[G * k : G * k + G, :])
                own = slice(G * part + LANES * k, G * part + LANES * k + LANES)
                rh_ref[0:G, own] = high
                rl_ref[0:G, own] = low_part
                swapped = slice(G * (1 - part) + LANES * k, G * (1 - part) + LANES * k + LANES)
                rh_ref[G : 2 * G, swapped] = high if part else -high
                rl_ref[G : 2 * G, swapped] = low_part if part else -low_part
        for t in range(3):
            cols = slice(256 * t, 256 * t + 256)
            out_ref[pair, :, cols] = (
                dot(ch_ref[...], rh_ref[:, cols]) + dot(cl_ref[...], rh_ref[:, cols]) + dot(ch_ref[...], rl_ref[:, cols])
            )


def y_transform(recv, ghost, ch, cl):
    return pl.pallas_call(
        y_kernel,
        out_shape=jax.ShapeDtypeStruct((3, G, 2 * G), F32),
        in_specs=[pl.BlockSpec(memory_space=pltpu.VMEM)] * 4,
        out_specs=pl.BlockSpec(memory_space=pltpu.VMEM),
        scratch_shapes=[pltpu.VMEM((3 * G, LANES), F32), pltpu.VMEM((2 * G, 2 * G), BF), pltpu.VMEM((2 * G, 2 * G), BF)],
        compiler_params=pltpu.CompilerParams(vmem_limit_bytes=40 * 1024 * 1024),
        name="y_transform",
    )(recv, ghost, ch, cl)


def z_kernel(in_ref, ch_ref, cl_ref, bc_ref, out_ref, sum_ref, rh_ref, rl_ref, lh_ref, ll_ref):
    lane = lax.broadcasted_iota(jnp.int32, (LEN_Z, LANES), 1)
    for src, dst in ((ch_ref, rh_ref), (cl_ref, rl_ref)):

        def place(first, rows, z, part):
            cos_part = src[z : z + rows, 0:G]
            sine_part = src[z : z + rows, G : 2 * G]
            dst[first : first + rows, 0:G] = sine_part if part else cos_part
            dst[first : first + rows, G : 2 * G] = cos_part if part else -sine_part

        for half in range(2):
            for part in range(2):
                place(LANES * (2 * half + part), LANES, LEN_Z * half, part)
                place(512 + LANES * half + 64 * part, 64, LEN_Z * half + LANES, part)
    total = jnp.zeros((8, G), F32)
    for pair in range(3):
        for odd in range(2):
            rows = slice(LEN_Z * odd, LEN_Z * odd + LEN_Z)

            def put(col, value):
                high, low = split(value)
                lh_ref[rows, col : col + LANES] = high
                ll_ref[rows, col : col + LANES] = low

            for half in range(2):
                highs = []
                for part in range(2):
                    first = G * part + LANES * odd
                    put(LANES * (2 * half + part), in_ref[half, pair, :, first : first + LANES])
                    highs.append(in_ref[half, pair, :, G * part + 256 : G * part + 384])
                if odd:
                    merged = jnp.where(lane < 64, pltpu.roll(highs[0], 64, 1), highs[1])
                else:
                    merged = jnp.where(lane < 64, highs[0], pltpu.roll(highs[1], 64, 1))
                put(512 + LANES * half, merged)
        mode = (
            dot(lh_ref[...], rh_ref[...]) + dot(ll_ref[...], rh_ref[...]) + dot(lh_ref[...], rl_ref[...])
        )
        for odd in range(2):
            real = mode[LEN_Z * odd : LEN_Z * odd + LEN_Z, 0:G]
            imag = mode[LEN_Z * odd : LEN_Z * odd + LEN_Z, G : 2 * G]
            value = 0.5 * bc_ref[2 * pair + odd] * (real * real + imag * imag)
            out_ref[2 * pair + odd] = value
            total = total + jnp.sum(value.reshape(LEN_Z // 8, 8, G), axis=0)
    sum_ref[...] = total


def z_transform(halves, ch, cl, influence):
    return pl.pallas_call(
        z_kernel,
        out_shape=(jax.ShapeDtypeStruct((6, LEN_Z, G), F32), jax.ShapeDtypeStruct((8, G), F32)),
        in_specs=[pl.BlockSpec(memory_space=pltpu.VMEM)] * 4,
        out_specs=(pl.BlockSpec(memory_space=pltpu.VMEM),) * 2,
        scratch_shapes=[pltpu.VMEM((2 * G, 2 * G), BF)] * 2 + [pltpu.VMEM((G, 2 * G), BF)] * 2,
        compiler_params=pltpu.CompilerParams(vmem_limit_bytes=40 * 1024 * 1024),
        name="z_transform",
    )(halves, ch, cl, influence)


def solution(mesh):
    slots = ('sys', 'ydom', 'zdom')
    mode_spec = P(('sys', 'ydom'), 'zdom', None)
    tables = twiddles()

    def local_energy(charge, real_mask, grid_idx, spline_w, influence):
        fh, fl, ch, cl = [jnp.asarray(table) for table in tables]
        w = jnp.transpose(spline_w, (1, 2, 0))
        idx = jnp.transpose(grid_idx, (1, 0))
        msg = spread(w, idx, charge[None, :], real_mask[None, :], fh, fl).reshape(NY, BLOCK, LANES)
        ghost = lax.ppermute(msg[:, 0:16, :], 'zdom', [(0, 1), (1, 0)])
        recv = lax.all_to_all(jnp.concatenate([msg, ghost], axis=1), 'ydom', 0, 0, tiled=True)
        ghost = recv[:, BLOCK:, :].reshape(NY * 16, LANES)
        planes = y_transform(recv[:, :BLOCK, :].reshape(NY * BLOCK, LANES), ghost, ch, cl)
        halves = lax.all_to_all(planes.reshape(3, 2, LEN_Z, 2 * G).transpose(1, 0, 2, 3), 'zdom', 0, 0, tiled=True)
        mode_energy, sums = z_transform(halves, ch, cl, influence)
        energy = lax.psum(jnp.sum(sums), ('ydom', 'zdom')) / (G * G * G)
        return mode_energy, jnp.reshape(energy, (1,))

    return jax.shard_map(local_energy, mesh=mesh, in_specs=(P(slots), P(slots), P(slots, None), P(slots, None, None), mode_spec), out_specs=(mode_spec, P('sys')), check_vma=False)
```

```python
import functools
import jax
import jax.numpy as jnp
import numpy as np
from jax import lax
from jax.experimental import pallas as pl
from jax.experimental.pallas import tpu as pltpu
from jax.sharding import PartitionSpec as P

G = 384
TAPS = 4
NY = 64
LEN_Y = 6
LEN_Z = 192
EXT_Y = 9
CHUNK = 512
LANES = 128
TILES = 14
COLS = TILES * LANES
ROWS = 12
BLOCK = ROWS * TILES
BF = jnp.bfloat16
F32 = jnp.float32
MESH = pl.DeviceIdType.MESH
FULL_SCALE = 32000.0
LOG_STEP = float(np.log(2.0) / 64.0)

LOW_TILE = 1
HIGH_TILE = 10


def split_np(table):
    high = table.astype(np.float32).astype(jnp.bfloat16)
    low = (table - high.astype(np.float64)).astype(np.float32).astype(jnp.bfloat16)
    return high, low


def twiddles():
    phase = (np.arange(G)[:, None] * np.arange(G)[None, :]) % G
    angle = phase * (2.0 * np.pi / G)
    cos_part, sine_part = np.cos(angle), np.sin(angle)
    freq = (6 * np.arange(NY)[None, :] + np.arange(6)[:, None]).reshape(-1)
    x_rows = np.concatenate([cos_part[freq], -sine_part[freq]], axis=0)
    both = np.concatenate([cos_part, sine_part], axis=1)
    return split_np(x_rows) + split_np(both)


def split(value):
    high = value.astype(BF)
    return high, (value - high.astype(F32)).astype(BF)


def level_code(largest):
    return jnp.clip(jnp.ceil(jnp.log(jnp.maximum(largest, 1e-30)) * (1.0 / LOG_STEP)), -8000.0, 8000.0)


def dot(a, b):
    return lax.dot_general(a, b, (((1,), (0,)), ((), ())), preferred_element_type=F32)


def dot_nt(a, b):
    return lax.dot_general(a, b, (((1,), (1,)), ((), ())), preferred_element_type=F32)


def row_iota(first, rows):
    return lax.broadcasted_iota(jnp.int32, (rows, CHUNK), 0) + first


def pick(rows, positions, weights):
    line = jnp.where(rows == positions[3], weights[3], 0.0)
    for s in (2, 1, 0):
        line = jnp.where(rows == positions[s], weights[s], line)
    return line


def spread_kernel(w_ref, idx_ref, q_ref, m_ref, fh_ref, fl_ref, msg_ref, acc_ref, lz_ref, qh_ref, ql_ref, modes_ref, rows_ref, *bufs):
    slots = q_ref.shape[1]

    def build(step, ah, al, bh, bl):
        span = pl.ds(pl.multiple_of(step * CHUNK, CHUNK), CHUNK)
        charge = q_ref[:, span] * m_ref[:, span].astype(F32)

        def rows16(value):
            return jnp.broadcast_to(value, (16, CHUNK))

        def taps(dim, scale, modulus):
            base = idx_ref[dim : dim + 1, span]
            positions, weights = [], []
            for s in range(TAPS):
                position = base + s
                if modulus is not None:
                    position = jnp.where(position >= modulus, position - modulus, position)
                weight = w_ref[dim, s : s + 1, span]
                positions.append(rows16(position))
                weights.append(rows16(weight if scale is None else weight * scale))
            return positions, weights

        pos_x, wgt_x = taps(0, charge, G)
        for g in range(G // 16):
            high, low = split(pick(row_iota(16 * g, 16), pos_x, wgt_x))
            ah[16 * g : 16 * g + 16, :] = high
            al[16 * g : 16 * g + 16, :] = low
        pos_z, wgt_z = taps(2, None, None)
        for g in range(LEN_Z // 16):
            lz_ref[16 * g : 16 * g + 16, :] = pick(row_iota(16 * g, 16), pos_z, wgt_z)
        pos_y, wgt_y = taps(1, None, None)
        for g in range(4):
            rows = row_iota(16 * g, 16)
            value = pick(lax.shift_right_logical(rows, 2), pos_y, wgt_y) * pick(
                LEN_Z + lax.bitwise_and(rows, 3), pos_z, wgt_z
            )
            high, low = split(value)
            bh[64 + 16 * g : 80 + 16 * g, :] = high
            bl[64 + 16 * g : 80 + 16 * g, :] = low
        for y in range(EXT_Y):
            line = pick(jnp.full((16, CHUNK), y, jnp.int32), pos_y, wgt_y)
            for g in range(LEN_Z // 16):
                if g < 8:
                    first = LANES * (LOW_TILE + y) + 16 * g
                elif y == 8:
                    first = 16 * (g - 8)
                else:
                    first = LANES * HIGH_TILE + 64 * y + 16 * (g - 8)
                high, low = split(lz_ref[16 * g : 16 * g + 16, :] * line)
                bh[first : first + 16, :] = high
                bl[first : first + 16, :] = low

    def accumulate(ah, al, bh, bl):
        for t in range(TILES // 2):
            cols = slice(256 * t, 256 * t + 256)
            part = dot_nt(ah[...], bh[cols, :]) + dot_nt(al[...], bh[cols, :]) + dot_nt(ah[...], bl[cols, :])
            acc_ref[:, cols] += part

    first, second = bufs[:4], bufs[4:]
    acc_ref[...] = jnp.zeros_like(acc_ref)
    build(0, *first)
    chunks = slots // CHUNK

    def body(pair, carry):
        accumulate(*first)
        build(2 * pair + 1, *second)
        accumulate(*second)
        build(jnp.minimum(2 * pair + 2, chunks - 1), *first)
        return carry

    lax.fori_loop(0, chunks // 2, body, 0)

    for t in range(TILES // 2):
        cols = slice(256 * t, 256 * t + 256)
        high, low = split(acc_ref[:, cols])
        qh_ref[:, cols] = high
        ql_ref[:, cols] = low
    for t in range(TILES // 2):
        cols = slice(256 * t, 256 * t + 256)
        part = dot(fh_ref[...], qh_ref[:, cols]) + dot(fl_ref[...], qh_ref[:, cols]) + dot(fh_ref[...], ql_ref[:, cols])
        modes_ref[:, cols] = part
        size = jnp.maximum(jnp.abs(part[:, :LANES]), jnp.abs(part[:, LANES:]))
        largest = size if t == 0 else jnp.maximum(largest, size)
    code = level_code(jnp.max(largest, axis=1, keepdims=True))
    inverse = jnp.exp(code * (-LOG_STEP)) * FULL_SCALE
    lane = lax.broadcasted_iota(jnp.int32, (ROWS * NY, LANES), 1)
    for t in range(TILES):
        value = modes_ref[:, LANES * t : LANES * t + LANES] * inverse
        if t == 0:
            value = jnp.where(lane == LANES - 1, code, value)
        for r in range(ROWS):
            rows_ref[pl.ds(t * ROWS + r, NY, stride=BLOCK), :] = value[NY * r : NY * r + NY, :]

    def pack(peer, carry):
        span = pl.ds(pl.multiple_of(peer * BLOCK, 8), BLOCK)
        value = lax.round(rows_ref[span, :], lax.RoundingMethod.TO_NEAREST_EVEN)
        msg_ref[peer] = value.astype(jnp.int32).astype(jnp.int16)
        return carry

    lax.fori_loop(0, NY, pack, 0)


def spread(w, idx, charge, mask, fh, fl):
    return pl.pallas_call(
        spread_kernel,
        out_shape=jax.ShapeDtypeStruct((NY, BLOCK, LANES), jnp.int16),
        in_specs=[pl.BlockSpec(memory_space=pltpu.VMEM)] * 6,
        out_specs=pl.BlockSpec(memory_space=pltpu.VMEM),
        scratch_shapes=[
            pltpu.VMEM((G, COLS), F32),
            pltpu.VMEM((LEN_Z, CHUNK), F32),
            pltpu.VMEM((G, COLS), BF),
            pltpu.VMEM((G, COLS), BF),
            pltpu.VMEM((ROWS * NY, COLS), F32),
            pltpu.VMEM((NY * BLOCK, LANES), F32),
        ]
        + [
            pltpu.VMEM((G, CHUNK), BF),
            pltpu.VMEM((G, CHUNK), BF),
            pltpu.VMEM((COLS, CHUNK), BF),
            pltpu.VMEM((COLS, CHUNK), BF),
        ]
        * 2,
        compiler_params=pltpu.CompilerParams(vmem_limit_bytes=60 * 1024 * 1024),
        name="spread",
    )(w, idx, charge, mask, fh, fl)


def exchange_kernel(msg_ref, recv_ref, ghost_ref, send_sem, recv_sem, ghost_send_sem, ghost_recv_sem):
    me, half = lax.axis_index("ydom"), lax.axis_index("zdom")
    barrier = pltpu.get_barrier_semaphore()

    def greet(peer, carry):
        for side in range(2):
            pl.semaphore_signal(barrier, inc=1, device_id={"ydom": peer, "zdom": side}, device_id_type=MESH)
        return carry

    lax.fori_loop(0, NY, greet, 0)
    pl.semaphore_wait(barrier, 2 * NY)

    def peer_of(step):
        shift = lax.rem(step * 23, NY)
        x = lax.rem(me + shift, 4)
        y = lax.rem(me // 4 + shift // 4, 4)
        z = lax.rem(me // 16 + shift // 16, 4)
        return x + 4 * y + 16 * z

    def send_ghost(step, carry):
        peer = peer_of(step)
        pltpu.make_async_remote_copy(
            src_ref=msg_ref.at[peer, pl.ds(0, 16)],
            dst_ref=ghost_ref.at[me],
            send_sem=ghost_send_sem,
            recv_sem=ghost_recv_sem,
            device_id={"ydom": peer, "zdom": 1 - half},
            device_id_type=MESH,
        ).start()
        return carry

    def send(step, carry):
        peer = peer_of(step)
        pltpu.make_async_remote_copy(
            src_ref=msg_ref.at[peer],
            dst_ref=recv_ref.at[me],
            send_sem=send_sem,
            recv_sem=recv_sem,
            device_id={"ydom": peer},
            device_id_type=MESH,
        ).start()
        return carry

    lax.fori_loop(1, NY, send, 0)
    lax.fori_loop(0, NY, send_ghost, 0)
    recv_ref[me] = msg_ref[me]
    others = pl.ds(0, NY - 1)
    pltpu.make_async_copy(recv_ref.at[others], recv_ref.at[others], recv_sem).wait()
    pltpu.make_async_copy(ghost_ref, ghost_ref, ghost_recv_sem).wait()
    pltpu.make_async_copy(recv_ref.at[others], recv_ref.at[others], send_sem).wait()
    pltpu.make_async_copy(ghost_ref, ghost_ref, ghost_send_sem).wait()


def exchange(msg):
    return pl.pallas_call(
        exchange_kernel,
        out_shape=(
            jax.ShapeDtypeStruct((NY, BLOCK, LANES), jnp.int16),
            jax.ShapeDtypeStruct((NY, 16, LANES), jnp.int16),
        ),
        in_specs=[pl.BlockSpec(memory_space=pltpu.VMEM)],
        out_specs=(pl.BlockSpec(memory_space=pltpu.VMEM),) * 2,
        scratch_shapes=[pltpu.SemaphoreType.DMA] * 4,
        compiler_params=pltpu.CompilerParams(
            vmem_limit_bytes=16 * 1024 * 1024, collective_id=0, has_side_effects=True
        ),
        name="exchange",
    )(msg)


def y_kernel(
    recv16_ref, ghost16_ref, ch_ref, cl_ref, own_ref, other_ref,
    recv_ref, ghost_ref, x_ref, rh_ref, rl_ref, away_ref, send_sems, recv_sems,
):
    side = lax.axis_index("zdom")
    barrier = pltpu.get_barrier_semaphore()
    pl.semaphore_signal(barrier, inc=1, device_id={"zdom": 1 - side}, device_id_type=MESH)

    def unpack(peer, carry):
        span = pl.ds(pl.multiple_of(peer * BLOCK, 8), BLOCK)
        recv_ref[span, :] = recv16_ref[peer].astype(jnp.int32).astype(F32)
        span = pl.ds(pl.multiple_of(peer * 16, 8), 16)
        ghost_ref[span, :] = ghost16_ref[peer].astype(jnp.int32).astype(F32)
        return carry

    lax.fori_loop(0, NY, unpack, 0)
    copies = []
    lane = lax.broadcasted_iota(jnp.int32, (NY, LANES), 1)

    def raw(t, row):
        return recv_ref[pl.ds(t * ROWS + row, NY, stride=BLOCK), :]

    def level(coded):
        return jnp.broadcast_to(jnp.exp(coded[:, LANES - 1 :] * LOG_STEP) * (1.0 / FULL_SCALE), (NY, LANES))

    def before(value):
        return pltpu.roll(value, 1, 0)

    def half_turn(value):
        return pltpu.roll(value, 64, 1)

    for pair in range(3):
        for part in range(2):
            high_tiles = []
            for odd in range(2):
                row = 6 * part + 2 * pair + odd
                edge = raw(0, row)
                scale = level(edge)
                edge = edge * scale
                ghost = ghost_ref[pl.ds(row, NY, stride=16), :]
                ghost = ghost * level(ghost)

                def tile(t, row):
                    return raw(t, row) * scale

                def low(y):
                    moved = pltpu.roll(ghost, LANES - 64 - 4 * y, 1)
                    return tile(LOW_TILE + y, row) + jnp.where(lane < 3, moved, 0.0)

                for y in range(LEN_Y):
                    value = low(y)
                    if y < 3:
                        value = value + before(low(y + 6))
                    x_ref[pl.ds(G * odd + y, NY, stride=LEN_Y), :] = value
                tiles = [tile(HIGH_TILE + k, row) for k in range(3)]
                tiles[0] = tiles[0] + before(tile(HIGH_TILE + 3, row))
                tiles[1] = tiles[1] + jnp.where(lane < 64, before(edge), 0.0)
                high_tiles.append(tiles)
            for k in range(3):
                even, odd = high_tiles[0][k], high_tiles[1][k]
                x_ref[pl.ds(2 * G + 2 * k, NY, stride=LEN_Y), :] = jnp.where(lane < 64, even, half_turn(odd))
                x_ref[pl.ds(2 * G + 2 * k + 1, NY, stride=LEN_Y), :] = jnp.where(lane < 64, half_turn(even), odd)
            for k in range(3):
                high, low_part = split(x_ref[G * k : G * k + G, :])
                own = slice(G * part + LANES * k, G * part + LANES * k + LANES)
                rh_ref[0:G, own] = high
                rl_ref[0:G, own] = low_part
                swapped = slice(G * (1 - part) + LANES * k, G * (1 - part) + LANES * k + LANES)
                rh_ref[G : 2 * G, swapped] = high if part else -high
                rl_ref[G : 2 * G, swapped] = low_part if part else -low_part
        for t in range(3):
            cols = slice(256 * t, 256 * t + 256)
            part = (
                dot(ch_ref[...], rh_ref[:, cols]) + dot(cl_ref[...], rh_ref[:, cols]) + dot(ch_ref[...], rl_ref[:, cols])
            )
            upper, lower = part[:LEN_Z], part[LEN_Z:]
            own_ref[pair, :, cols] = jnp.where(side == 0, upper, lower)
            away_ref[pair, :, cols] = jnp.where(side == 0, lower, upper)
        if pair == 0:
            pl.semaphore_wait(barrier, 1)
        copies.append(
            pltpu.make_async_remote_copy(
                src_ref=away_ref.at[pair],
                dst_ref=other_ref.at[pair],
                send_sem=send_sems.at[pair],
                recv_sem=recv_sems.at[pair],
                device_id={"zdom": 1 - side},
                device_id_type=MESH,
            )
        )
        copies[-1].start()
    for copy in copies:
        copy.wait()


def y_transform(recv, ghost, ch, cl):
    half = jax.ShapeDtypeStruct((3, LEN_Z, 2 * G), F32)
    return pl.pallas_call(
        y_kernel,
        out_shape=(half, half),
        in_specs=[pl.BlockSpec(memory_space=pltpu.VMEM)] * 4,
        out_specs=(pl.BlockSpec(memory_space=pltpu.VMEM),) * 2,
        scratch_shapes=[
            pltpu.VMEM((NY * BLOCK, LANES), F32),
            pltpu.VMEM((NY * 16, LANES), F32),
            pltpu.VMEM((3 * G, LANES), F32),
            pltpu.VMEM((2 * G, 2 * G), BF),
            pltpu.VMEM((2 * G, 2 * G), BF),
            pltpu.VMEM((3, LEN_Z, 2 * G), F32),
            pltpu.SemaphoreType.DMA((3,)),
            pltpu.SemaphoreType.DMA((3,)),
        ],
        compiler_params=pltpu.CompilerParams(
            vmem_limit_bytes=40 * 1024 * 1024, collective_id=1, has_side_effects=True
        ),
        name="y_transform",
    )(recv, ghost, ch, cl)


def z_kernel(
    own_ref, other_ref, ch_ref, cl_ref, bc_ref, out_ref, sum_ref,
    rh_ref, rl_ref, lh_ref, ll_ref, part_ref, parts_ref, pair_ref, sems,
):
    me, side = lax.axis_index("ydom"), lax.axis_index("zdom")
    barrier = pltpu.get_barrier_semaphore()

    def greet(step, carry):
        pl.semaphore_signal(barrier, inc=1, device_id={"ydom": lax.rem(me + step, NY)}, device_id_type=MESH)
        return carry

    lax.fori_loop(1, NY, greet, 0)
    pl.semaphore_signal(barrier, inc=1, device_id={"zdom": 1 - side}, device_id_type=MESH)
    lane = lax.broadcasted_iota(jnp.int32, (LEN_Z, LANES), 1)
    for src, dst in ((ch_ref, rh_ref), (cl_ref, rl_ref)):

        def place(first, rows, half, z, part):
            span = pl.ds(pl.multiple_of(LEN_Z * (side if half == 0 else 1 - side) + z, 64), rows)
            cos_part = src[span, 0:G]
            sine_part = src[span, G : 2 * G]
            dst[first : first + rows, 0:G] = sine_part if part else cos_part
            dst[first : first + rows, G : 2 * G] = cos_part if part else -sine_part

        for half in range(2):
            for part in range(2):
                place(LANES * (2 * half + part), LANES, half, 0, part)
                place(512 + LANES * half + 64 * part, 64, half, LANES, part)
    total = jnp.zeros((8, G), F32)
    for pair in range(3):
        for odd in range(2):
            rows = slice(LEN_Z * odd, LEN_Z * odd + LEN_Z)

            def put(col, value):
                high, low = split(value)
                lh_ref[rows, col : col + LANES] = high
                ll_ref[rows, col : col + LANES] = low

            for half, in_ref in enumerate((own_ref, other_ref)):
                highs = []
                for part in range(2):
                    first = G * part + LANES * odd
                    put(LANES * (2 * half + part), in_ref[pair, :, first : first + LANES])
                    highs.append(in_ref[pair, :, G * part + 256 : G * part + 384])
                if odd:
                    merged = jnp.where(lane < 64, pltpu.roll(highs[0], 64, 1), highs[1])
                else:
                    merged = jnp.where(lane < 64, highs[0], pltpu.roll(highs[1], 64, 1))
                put(512 + LANES * half, merged)
        mode = (
            dot(lh_ref[...], rh_ref[...]) + dot(ll_ref[...], rh_ref[...]) + dot(lh_ref[...], rl_ref[...])
        )
        for odd in range(2):
            real = mode[LEN_Z * odd : LEN_Z * odd + LEN_Z, 0:G]
            imag = mode[LEN_Z * odd : LEN_Z * odd + LEN_Z, G : 2 * G]
            value = 0.5 * bc_ref[2 * pair + odd] * (real * real + imag * imag)
            out_ref[2 * pair + odd] = value
            total = total + jnp.sum(value.reshape(LEN_Z // 8, 8, G), axis=0)
    lanes = total[:, :LANES] + total[:, LANES : 2 * LANES] + total[:, 2 * LANES :]
    part_ref[...] = jnp.sum(lanes, axis=0, keepdims=True)
    pl.semaphore_wait(barrier, NY)

    def send(step, carry):
        pltpu.make_async_remote_copy(
            src_ref=part_ref,
            dst_ref=parts_ref.at[me],
            send_sem=sems.at[0],
            recv_sem=sems.at[1],
            device_id={"ydom": lax.rem(me + step, NY)},
            device_id_type=MESH,
        ).start()
        return carry

    lax.fori_loop(1, NY, send, 0)
    parts_ref[me] = part_ref[...]
    others = pl.ds(0, NY - 1)
    pltpu.make_async_copy(parts_ref.at[others], parts_ref.at[others], sems.at[1]).wait()
    pltpu.make_async_copy(parts_ref.at[others], parts_ref.at[others], sems.at[0]).wait()
    pair_ref[0] = jnp.sum(parts_ref[...], axis=0)
    copy = pltpu.make_async_remote_copy(
        src_ref=pair_ref.at[0],
        dst_ref=pair_ref.at[1],
        send_sem=sems.at[2],
        recv_sem=sems.at[3],
        device_id={"zdom": 1 - side},
        device_id_type=MESH,
    )
    copy.start()
    copy.wait()
    energy = jnp.sum(pair_ref[0] + pair_ref[1], axis=1, keepdims=True) * (1.0 / (G * G * G))
    sum_ref[...] = jnp.broadcast_to(energy, (1, LANES))


def z_transform(own, other, ch, cl, influence):
    return pl.pallas_call(
        z_kernel,
        out_shape=(jax.ShapeDtypeStruct((6, LEN_Z, G), F32), jax.ShapeDtypeStruct((1, LANES), F32)),
        in_specs=[pl.BlockSpec(memory_space=pltpu.VMEM)] * 5,
        out_specs=(pl.BlockSpec(memory_space=pltpu.VMEM),) * 2,
        scratch_shapes=[pltpu.VMEM((2 * G, 2 * G), BF)] * 2
        + [pltpu.VMEM((G, 2 * G), BF)] * 2
        + [
            pltpu.VMEM((1, LANES), F32),
            pltpu.VMEM((NY, 1, LANES), F32),
            pltpu.VMEM((2, 1, LANES), F32),
            pltpu.SemaphoreType.DMA((4,)),
        ],
        compiler_params=pltpu.CompilerParams(
            vmem_limit_bytes=40 * 1024 * 1024, collective_id=2, has_side_effects=True
        ),
        name="z_transform",
    )(own, other, ch, cl, influence)


def solution(mesh):
    slots = ('sys', 'ydom', 'zdom')
    mode_spec = P(('sys', 'ydom'), 'zdom', None)
    tables = twiddles()

    def local_energy(charge, real_mask, grid_idx, spline_w, influence):
        fh, fl, ch, cl = [jnp.asarray(table) for table in tables]
        w = jnp.transpose(spline_w, (1, 2, 0))
        idx = jnp.transpose(grid_idx, (1, 0))
        msg = spread(w, idx, charge[None, :], real_mask[None, :], fh, fl)
        recv, ghost = exchange(msg)
        own, other = y_transform(recv, ghost, ch, cl)
        mode_energy, energy = z_transform(own, other, ch, cl, influence)
        return mode_energy, energy[0, :1]

    return jax.shard_map(local_energy, mesh=mesh, in_specs=(P(slots), P(slots), P(slots, None), P(slots, None, None), mode_spec), out_specs=(mode_spec, P('sys')), check_vma=False)
```

```python
import functools
import jax
import jax.numpy as jnp
import numpy as np
from jax import lax
from jax.experimental import pallas as pl
from jax.experimental.pallas import tpu as pltpu
from jax.sharding import PartitionSpec as P

G = 384
TAPS = 4
NY = 64
LEN_Y = 6
LEN_Z = 192
EXT_Y = 9
CHUNK = 256
WINDOW = 128
X_ROWS = 520
LANES = 128
TILES = 14
COLS = TILES * LANES
ROWS = 12
BLOCK = ROWS * TILES
BF = jnp.bfloat16
F32 = jnp.float32
MESH = pl.DeviceIdType.MESH
FULL_SCALE = 32000.0
LOG_STEP = float(np.log(2.0) / 64.0)

LOW_TILE = 1
HIGH_TILE = 10


def split_np(table):
    high = table.astype(np.float32).astype(jnp.bfloat16)
    low = (table - high.astype(np.float64)).astype(np.float32).astype(jnp.bfloat16)
    return high, low


def twiddles():
    phase = (np.arange(G)[:, None] * np.arange(G)[None, :]) % G
    angle = phase * (2.0 * np.pi / G)
    cos_part, sine_part = np.cos(angle), np.sin(angle)
    freq = (6 * np.arange(NY)[None, :] + np.arange(6)[:, None]).reshape(-1)
    x_rows = np.concatenate([cos_part[freq], -sine_part[freq]], axis=0)
    both = np.concatenate([cos_part, sine_part], axis=1)
    return split_np(x_rows) + split_np(both)


def split(value):
    high = value.astype(BF)
    return high, (value - high.astype(F32)).astype(BF)


def level_code(largest):
    return jnp.clip(jnp.ceil(jnp.log(jnp.maximum(largest, 1e-30)) * (1.0 / LOG_STEP)), -8000.0, 8000.0)


def dot(a, b):
    return lax.dot_general(a, b, (((1,), (0,)), ((), ())), preferred_element_type=F32)


def dot_nt(a, b):
    return lax.dot_general(a, b, (((1,), (1,)), ((), ())), preferred_element_type=F32)


def row_iota(first, rows):
    return lax.broadcasted_iota(jnp.int32, (rows, CHUNK), 0) + first


def pick(rows, positions, weights):
    line = jnp.where(rows == positions[3], weights[3], 0.0)
    for s in (2, 1, 0):
        line = jnp.where(rows == positions[s], weights[s], line)
    return line


def sort_lanes(key):
    lane = lax.broadcasted_iota(jnp.int32, key.shape, 1)
    size = 2
    while size <= LANES:
        distance = size // 2
        while distance:
            lower = lax.bitwise_and(lane, distance) == 0
            other = jnp.where(lower, pltpu.roll(key, LANES - distance, 1), pltpu.roll(key, distance, 1))
            ascending = lax.bitwise_and(lane, size) == 0
            key = jnp.where(lower == ascending, jnp.minimum(key, other), jnp.maximum(key, other))
            distance //= 2
        size *= 2
    return key


def spread_kernel(
    w_ref, idx_ref, q_ref, m_ref, fh_ref, fl_ref, msg_ref,
    acc_ref, lz_ref, qh_ref, ql_ref, modes_ref, rows_ref, wgt_ref, base_ref, spare_ref, *bufs,
):
    lane = lax.broadcasted_iota(jnp.int32, (LANES, LANES), 1)
    key = sort_lanes((idx_ref[0] * LANES + lane).astype(F32)).astype(jnp.int32)
    order = lax.bitwise_and(key, LANES - 1)

    def place(value):
        return jnp.transpose(jnp.take_along_axis(value, order, axis=1))

    base_ref[0] = jnp.transpose(lax.shift_right_logical(key, 7))
    base_ref[1] = place(idx_ref[1])
    base_ref[2] = place(idx_ref[2])
    charge = q_ref[...] * m_ref[...].astype(F32)
    for dim in range(3):
        for s in range(TAPS):
            value = w_ref[TAPS * dim + s]
            wgt_ref[TAPS * dim + s] = place(value * charge if dim == 0 else value)

    def row_of(ref, field, step):
        pieces = [
            jnp.broadcast_to(ref[field, pl.ds(2 * step + k, 1), :], (16, LANES)) for k in range(2)
        ]
        return jnp.concatenate(pieces, axis=1)

    def taps(dim, step, first):
        base = row_of(base_ref, dim, step) - first
        return [base + s for s in range(TAPS)], [row_of(wgt_ref, TAPS * dim + s, step) for s in range(TAPS)]

    def build_x(step, first, a):
        pos_x, wgt_x = taps(0, step, first)
        for g in range(WINDOW // 16):
            high, low = split(pick(row_iota(16 * g, 16), pos_x, wgt_x))
            a[16 * g : 16 * g + 16, :] = high
            a[WINDOW + 16 * g : WINDOW + 16 * g + 16, :] = low

    def build(step, a, bh, bl):
        bases = base_ref[0, pl.ds(2 * step, 2), :]
        first = jnp.min(bases) // 8 * 8
        windows = (jnp.max(bases) + 3 - first) // WINDOW + 1
        build_x(step, first, a)
        pos_z, wgt_z = taps(2, step, 0)
        for g in range(LEN_Z // 16):
            lz_ref[16 * g : 16 * g + 16, :] = pick(row_iota(16 * g, 16), pos_z, wgt_z)
        pos_y, wgt_y = taps(1, step, 0)
        for g in range(4):
            rows = row_iota(16 * g, 16)
            value = pick(lax.shift_right_logical(rows, 2), pos_y, wgt_y) * pick(
                LEN_Z + lax.bitwise_and(rows, 3), pos_z, wgt_z
            )
            high, low = split(value)
            bh[64 + 16 * g : 80 + 16 * g, :] = high
            bl[64 + 16 * g : 80 + 16 * g, :] = low
        for y in range(EXT_Y):
            line = pick(jnp.full((16, CHUNK), y, jnp.int32), pos_y, wgt_y)
            for g in range(LEN_Z // 16):
                if g < 8:
                    row = LANES * (LOW_TILE + y) + 16 * g
                elif y == 8:
                    row = 16 * (g - 8)
                else:
                    row = LANES * HIGH_TILE + 64 * y + 16 * (g - 8)
                high, low = split(lz_ref[16 * g : 16 * g + 16, :] * line)
                bh[row : row + 16, :] = high
                bl[row : row + 16, :] = low
        return first, windows

    def accumulate(first, a, bh, bl):
        span = pl.ds(pl.multiple_of(first, 8), WINDOW)
        for t in range(TILES // 2):
            cols = slice(256 * t, 256 * t + 256)
            both = dot_nt(a[...], bh[cols, :])
            acc_ref[span, cols] += both[:WINDOW] + both[WINDOW:] + dot_nt(a[:WINDOW, :], bl[cols, :])

    def remaining(step, first, windows, a, bh, bl):
        def window(k, carry):
            build_x(step, first + WINDOW * k, spare_ref)
            accumulate(first + WINDOW * k, spare_ref, bh, bl)
            return carry

        lax.fori_loop(1, windows, window, 0)

    one, two = bufs[:3], bufs[3:]
    acc_ref[...] = jnp.zeros_like(acc_ref)
    chunks = LANES * LANES // CHUNK

    def body(pair, carry):
        first, windows = carry
        accumulate(first, *one)
        next_first, next_windows = build(2 * pair + 1, *two)
        remaining(2 * pair, first, windows, *one)
        accumulate(next_first, *two)
        carry = build(jnp.minimum(2 * pair + 2, chunks - 1), *one)
        remaining(2 * pair + 1, next_first, next_windows, *two)
        return carry

    lax.fori_loop(0, chunks // 2, body, build(0, *one))
    acc_ref[0:8, :] += acc_ref[G : G + 8, :]

    for t in range(TILES // 2):
        cols = slice(256 * t, 256 * t + 256)
        high, low = split(acc_ref[:G, cols])
        qh_ref[:, cols] = high
        ql_ref[:, cols] = low
    for t in range(TILES // 2):
        cols = slice(256 * t, 256 * t + 256)
        part = dot(fh_ref[...], qh_ref[:, cols]) + dot(fl_ref[...], qh_ref[:, cols]) + dot(fh_ref[...], ql_ref[:, cols])
        modes_ref[:, cols] = part
        size = jnp.maximum(jnp.abs(part[:, :LANES]), jnp.abs(part[:, LANES:]))
        largest = size if t == 0 else jnp.maximum(largest, size)
    code = level_code(jnp.max(largest, axis=1, keepdims=True))
    inverse = jnp.exp(code * (-LOG_STEP)) * FULL_SCALE
    lane = lax.broadcasted_iota(jnp.int32, (ROWS * NY, LANES), 1)
    for t in range(TILES):
        value = modes_ref[:, LANES * t : LANES * t + LANES] * inverse
        if t == 0:
            value = jnp.where(lane == LANES - 1, code, value)
        for r in range(ROWS):
            rows_ref[pl.ds(t * ROWS + r, NY, stride=BLOCK), :] = value[NY * r : NY * r + NY, :]

    def pack(peer, carry):
        span = pl.ds(pl.multiple_of(peer * BLOCK, 8), BLOCK)
        value = lax.round(rows_ref[span, :], lax.RoundingMethod.TO_NEAREST_EVEN)
        msg_ref[peer] = value.astype(jnp.int32).astype(jnp.int16)
        return carry

    lax.fori_loop(0, NY, pack, 0)


def spread(w, idx, charge, mask, fh, fl):
    return pl.pallas_call(
        spread_kernel,
        out_shape=jax.ShapeDtypeStruct((NY, BLOCK, LANES), jnp.int16),
        in_specs=[pl.BlockSpec(memory_space=pltpu.VMEM)] * 6,
        out_specs=pl.BlockSpec(memory_space=pltpu.VMEM),
        scratch_shapes=[
            pltpu.VMEM((X_ROWS, COLS), F32),
            pltpu.VMEM((LEN_Z, CHUNK), F32),
            pltpu.VMEM((G, COLS), BF),
            pltpu.VMEM((G, COLS), BF),
            pltpu.VMEM((ROWS * NY, COLS), F32),
            pltpu.VMEM((NY * BLOCK, LANES), F32),
        ]
        + [
            pltpu.VMEM((3 * TAPS, LANES, LANES), F32),
            pltpu.VMEM((3, LANES, LANES), jnp.int32),
            pltpu.VMEM((2 * WINDOW, CHUNK), BF),
        ]
        + [
            pltpu.VMEM((2 * WINDOW, CHUNK), BF),
            pltpu.VMEM((COLS, CHUNK), BF),
            pltpu.VMEM((COLS, CHUNK), BF),
        ]
        * 2,
        compiler_params=pltpu.CompilerParams(vmem_limit_bytes=60 * 1024 * 1024),
        name="spread",
    )(w, idx, charge, mask, fh, fl)


def exchange_kernel(msg_ref, recv_ref, ghost_ref, send_sem, recv_sem, ghost_send_sem, ghost_recv_sem):
    me, half = lax.axis_index("ydom"), lax.axis_index("zdom")
    barrier = pltpu.get_barrier_semaphore()

    def greet(peer, carry):
        for side in range(2):
            pl.semaphore_signal(barrier, inc=1, device_id={"ydom": peer, "zdom": side}, device_id_type=MESH)
        return carry

    lax.fori_loop(0, NY, greet, 0)
    pl.semaphore_wait(barrier, 2 * NY)

    def peer_of(step):
        shift = lax.rem(step * 23, NY)
        x = lax.rem(me + shift, 4)
        y = lax.rem(me // 4 + shift // 4, 4)
        z = lax.rem(me // 16 + shift // 16, 4)
        return x + 4 * y + 16 * z

    def send_ghost(step, carry):
        peer = peer_of(step)
        pltpu.make_async_remote_copy(
            src_ref=msg_ref.at[peer, pl.ds(0, 16)],
            dst_ref=ghost_ref.at[me],
            send_sem=ghost_send_sem,
            recv_sem=ghost_recv_sem,
            device_id={"ydom": peer, "zdom": 1 - half},
            device_id_type=MESH,
        ).start()
        return carry

    def send(step, carry):
        peer = peer_of(step)
        pltpu.make_async_remote_copy(
            src_ref=msg_ref.at[peer],
            dst_ref=recv_ref.at[me],
            send_sem=send_sem,
            recv_sem=recv_sem,
            device_id={"ydom": peer},
            device_id_type=MESH,
        ).start()
        return carry

    lax.fori_loop(1, NY, send, 0)
    lax.fori_loop(0, NY, send_ghost, 0)
    recv_ref[me] = msg_ref[me]
    others = pl.ds(0, NY - 1)
    pltpu.make_async_copy(recv_ref.at[others], recv_ref.at[others], recv_sem).wait()
    pltpu.make_async_copy(ghost_ref, ghost_ref, ghost_recv_sem).wait()
    pltpu.make_async_copy(recv_ref.at[others], recv_ref.at[others], send_sem).wait()
    pltpu.make_async_copy(ghost_ref, ghost_ref, ghost_send_sem).wait()


def exchange(msg):
    return pl.pallas_call(
        exchange_kernel,
        out_shape=(
            jax.ShapeDtypeStruct((NY, BLOCK, LANES), jnp.int16),
            jax.ShapeDtypeStruct((NY, 16, LANES), jnp.int16),
        ),
        in_specs=[pl.BlockSpec(memory_space=pltpu.VMEM)],
        out_specs=(pl.BlockSpec(memory_space=pltpu.VMEM),) * 2,
        scratch_shapes=[pltpu.SemaphoreType.DMA] * 4,
        compiler_params=pltpu.CompilerParams(
            vmem_limit_bytes=16 * 1024 * 1024, collective_id=0, has_side_effects=True
        ),
        name="exchange",
    )(msg)


def y_kernel(
    recv16_ref, ghost16_ref, ch_ref, cl_ref, own_ref, other_ref,
    recv_ref, ghost_ref, x_ref, rh_ref, rl_ref, away_ref, send_sems, recv_sems,
):
    side = lax.axis_index("zdom")
    barrier = pltpu.get_barrier_semaphore()
    pl.semaphore_signal(barrier, inc=1, device_id={"zdom": 1 - side}, device_id_type=MESH)

    def unpack(peer, carry):
        span = pl.ds(pl.multiple_of(peer * BLOCK, 8), BLOCK)
        recv_ref[span, :] = recv16_ref[peer].astype(jnp.int32).astype(F32)
        span = pl.ds(pl.multiple_of(peer * 16, 8), 16)
        ghost_ref[span, :] = ghost16_ref[peer].astype(jnp.int32).astype(F32)
        return carry

    lax.fori_loop(0, NY, unpack, 0)
    copies = []
    lane = lax.broadcasted_iota(jnp.int32, (NY, LANES), 1)

    def raw(t, row):
        return recv_ref[pl.ds(t * ROWS + row, NY, stride=BLOCK), :]

    def level(coded):
        return jnp.broadcast_to(jnp.exp(coded[:, LANES - 1 :] * LOG_STEP) * (1.0 / FULL_SCALE), (NY, LANES))

    def before(value):
        return pltpu.roll(value, 1, 0)

    def half_turn(value):
        return pltpu.roll(value, 64, 1)

    for pair in range(3):
        for part in range(2):
            high_tiles = []
            for odd in range(2):
                row = 6 * part + 2 * pair + odd
                edge = raw(0, row)
                scale = level(edge)
                edge = edge * scale
                ghost = ghost_ref[pl.ds(row, NY, stride=16), :]
                ghost = ghost * level(ghost)

                def tile(t, row):
                    return raw(t, row) * scale

                def low(y):
                    moved = pltpu.roll(ghost, LANES - 64 - 4 * y, 1)
                    return tile(LOW_TILE + y, row) + jnp.where(lane < 3, moved, 0.0)

                for y in range(LEN_Y):
                    value = low(y)
                    if y < 3:
                        value = value + before(low(y + 6))
                    x_ref[pl.ds(G * odd + y, NY, stride=LEN_Y), :] = value
                tiles = [tile(HIGH_TILE + k, row) for k in range(3)]
                tiles[0] = tiles[0] + before(tile(HIGH_TILE + 3, row))
                tiles[1] = tiles[1] + jnp.where(lane < 64, before(edge), 0.0)
                high_tiles.append(tiles)
            for k in range(3):
                even, odd = high_tiles[0][k], high_tiles[1][k]
                x_ref[pl.ds(2 * G + 2 * k, NY, stride=LEN_Y), :] = jnp.where(lane < 64, even, half_turn(odd))
                x_ref[pl.ds(2 * G + 2 * k + 1, NY, stride=LEN_Y), :] = jnp.where(lane < 64, half_turn(even), odd)
            for k in range(3):
                high, low_part = split(x_ref[G * k : G * k + G, :])
                own = slice(G * part + LANES * k, G * part + LANES * k + LANES)
                rh_ref[0:G, own] = high
                rl_ref[0:G, own] = low_part
                swapped = slice(G * (1 - part) + LANES * k, G * (1 - part) + LANES * k + LANES)
                rh_ref[G : 2 * G, swapped] = high if part else -high
                rl_ref[G : 2 * G, swapped] = low_part if part else -low_part
        for t in range(3):
            cols = slice(256 * t, 256 * t + 256)
            part = (
                dot(ch_ref[...], rh_ref[:, cols]) + dot(cl_ref[...], rh_ref[:, cols]) + dot(ch_ref[...], rl_ref[:, cols])
            )
            upper, lower = part[:LEN_Z], part[LEN_Z:]
            own_ref[pair, :, cols] = jnp.where(side == 0, upper, lower)
            away_ref[pair, :, cols] = jnp.where(side == 0, lower, upper)
        if pair == 0:
            pl.semaphore_wait(barrier, 1)
        copies.append(
            pltpu.make_async_remote_copy(
                src_ref=away_ref.at[pair],
                dst_ref=other_ref.at[pair],
                send_sem=send_sems.at[pair],
                recv_sem=recv_sems.at[pair],
                device_id={"zdom": 1 - side},
                device_id_type=MESH,
            )
        )
        copies[-1].start()
    for copy in copies:
        copy.wait()


def y_transform(recv, ghost, ch, cl):
    half = jax.ShapeDtypeStruct((3, LEN_Z, 2 * G), F32)
    return pl.pallas_call(
        y_kernel,
        out_shape=(half, half),
        in_specs=[pl.BlockSpec(memory_space=pltpu.VMEM)] * 4,
        out_specs=(pl.BlockSpec(memory_space=pltpu.VMEM),) * 2,
        scratch_shapes=[
            pltpu.VMEM((NY * BLOCK, LANES), F32),
            pltpu.VMEM((NY * 16, LANES), F32),
            pltpu.VMEM((3 * G, LANES), F32),
            pltpu.VMEM((2 * G, 2 * G), BF),
            pltpu.VMEM((2 * G, 2 * G), BF),
            pltpu.VMEM((3, LEN_Z, 2 * G), F32),
            pltpu.SemaphoreType.DMA((3,)),
            pltpu.SemaphoreType.DMA((3,)),
        ],
        compiler_params=pltpu.CompilerParams(
            vmem_limit_bytes=40 * 1024 * 1024, collective_id=1, has_side_effects=True
        ),
        name="y_transform",
    )(recv, ghost, ch, cl)


def z_kernel(
    own_ref, other_ref, ch_ref, cl_ref, bc_ref, out_ref, sum_ref,
    rh_ref, rl_ref, lh_ref, ll_ref, part_ref, parts_ref, pair_ref, sems,
):
    me, side = lax.axis_index("ydom"), lax.axis_index("zdom")
    barrier = pltpu.get_barrier_semaphore()

    def greet(step, carry):
        pl.semaphore_signal(barrier, inc=1, device_id={"ydom": lax.rem(me + step, NY)}, device_id_type=MESH)
        return carry

    lax.fori_loop(1, NY, greet, 0)
    pl.semaphore_signal(barrier, inc=1, device_id={"zdom": 1 - side}, device_id_type=MESH)
    lane = lax.broadcasted_iota(jnp.int32, (LEN_Z, LANES), 1)
    for src, dst in ((ch_ref, rh_ref), (cl_ref, rl_ref)):

        def place(first, rows, half, z, part):
            span = pl.ds(pl.multiple_of(LEN_Z * (side if half == 0 else 1 - side) + z, 64), rows)
            cos_part = src[span, 0:G]
            sine_part = src[span, G : 2 * G]
            dst[first : first + rows, 0:G] = sine_part if part else cos_part
            dst[first : first + rows, G : 2 * G] = cos_part if part else -sine_part

        for half in range(2):
            for part in range(2):
                place(LANES * (2 * half + part), LANES, half, 0, part)
                place(512 + LANES * half + 64 * part, 64, half, LANES, part)
    total = jnp.zeros((8, G), F32)
    for pair in range(3):
        for odd in range(2):
            rows = slice(LEN_Z * odd, LEN_Z * odd + LEN_Z)

            def put(col, value):
                high, low = split(value)
                lh_ref[rows, col : col + LANES] = high
                ll_ref[rows, col : col + LANES] = low

            for half, in_ref in enumerate((own_ref, other_ref)):
                highs = []
                for part in range(2):
                    first = G * part + LANES * odd
                    put(LANES * (2 * half + part), in_ref[pair, :, first : first + LANES])
                    highs.append(in_ref[pair, :, G * part + 256 : G * part + 384])
                if odd:
                    merged = jnp.where(lane < 64, pltpu.roll(highs[0], 64, 1), highs[1])
                else:
                    merged = jnp.where(lane < 64, highs[0], pltpu.roll(highs[1], 64, 1))
                put(512 + LANES * half, merged)
        mode = (
            dot(lh_ref[...], rh_ref[...]) + dot(ll_ref[...], rh_ref[...]) + dot(lh_ref[...], rl_ref[...])
        )
        for odd in range(2):
            real = mode[LEN_Z * odd : LEN_Z * odd + LEN_Z, 0:G]
            imag = mode[LEN_Z * odd : LEN_Z * odd + LEN_Z, G : 2 * G]
            value = 0.5 * bc_ref[2 * pair + odd] * (real * real + imag * imag)
            out_ref[2 * pair + odd] = value
            total = total + jnp.sum(value.reshape(LEN_Z // 8, 8, G), axis=0)
    lanes = total[:, :LANES] + total[:, LANES : 2 * LANES] + total[:, 2 * LANES :]
    part_ref[...] = jnp.sum(lanes, axis=0, keepdims=True)
    pl.semaphore_wait(barrier, NY)

    def send(step, carry):
        pltpu.make_async_remote_copy(
            src_ref=part_ref,
            dst_ref=parts_ref.at[me],
            send_sem=sems.at[0],
            recv_sem=sems.at[1],
            device_id={"ydom": lax.rem(me + step, NY)},
            device_id_type=MESH,
        ).start()
        return carry

    lax.fori_loop(1, NY, send, 0)
    parts_ref[me] = part_ref[...]
    others = pl.ds(0, NY - 1)
    pltpu.make_async_copy(parts_ref.at[others], parts_ref.at[others], sems.at[1]).wait()
    pltpu.make_async_copy(parts_ref.at[others], parts_ref.at[others], sems.at[0]).wait()
    pair_ref[0] = jnp.sum(parts_ref[...], axis=0)
    copy = pltpu.make_async_remote_copy(
        src_ref=pair_ref.at[0],
        dst_ref=pair_ref.at[1],
        send_sem=sems.at[2],
        recv_sem=sems.at[3],
        device_id={"zdom": 1 - side},
        device_id_type=MESH,
    )
    copy.start()
    copy.wait()
    energy = jnp.sum(pair_ref[0] + pair_ref[1], axis=1, keepdims=True) * (1.0 / (G * G * G))
    sum_ref[...] = jnp.broadcast_to(energy, (1, LANES))


def z_transform(own, other, ch, cl, influence):
    return pl.pallas_call(
        z_kernel,
        out_shape=(jax.ShapeDtypeStruct((6, LEN_Z, G), F32), jax.ShapeDtypeStruct((1, LANES), F32)),
        in_specs=[pl.BlockSpec(memory_space=pltpu.VMEM)] * 5,
        out_specs=(pl.BlockSpec(memory_space=pltpu.VMEM),) * 2,
        scratch_shapes=[pltpu.VMEM((2 * G, 2 * G), BF)] * 2
        + [pltpu.VMEM((G, 2 * G), BF)] * 2
        + [
            pltpu.VMEM((1, LANES), F32),
            pltpu.VMEM((NY, 1, LANES), F32),
            pltpu.VMEM((2, 1, LANES), F32),
            pltpu.SemaphoreType.DMA((4,)),
        ],
        compiler_params=pltpu.CompilerParams(
            vmem_limit_bytes=40 * 1024 * 1024, collective_id=2, has_side_effects=True
        ),
        name="z_transform",
    )(own, other, ch, cl, influence)


def solution(mesh):
    slots = ('sys', 'ydom', 'zdom')
    mode_spec = P(('sys', 'ydom'), 'zdom', None)
    tables = twiddles()

    def local_energy(charge, real_mask, grid_idx, spline_w, influence):
        fh, fl, ch, cl = [jnp.asarray(table) for table in tables]
        square = (LANES, LANES)
        w = jnp.transpose(spline_w, (1, 2, 0)).reshape(3 * TAPS, *square)
        idx = jnp.transpose(grid_idx, (1, 0)).reshape(3, *square)
        msg = spread(w, idx, charge.reshape(square), real_mask.reshape(square), fh, fl)
        recv, ghost = exchange(msg)
        own, other = y_transform(recv, ghost, ch, cl)
        mode_energy, energy = z_transform(own, other, ch, cl, influence)
        return mode_energy, energy[0, :1]

    return jax.shard_map(local_energy, mesh=mesh, in_specs=(P(slots), P(slots), P(slots, None), P(slots, None, None), mode_spec), out_specs=(mode_spec, P('sys')), check_vma=False)
```

```python
import functools
import jax
import jax.numpy as jnp
import numpy as np
from jax import lax
from jax.experimental import pallas as pl
from jax.experimental.pallas import tpu as pltpu
from jax.sharding import PartitionSpec as P

G = 384
TAPS = 4
NY = 64
LEN_Y = 6
LEN_Z = 192
EXT_Y = 9
CHUNK = 256
WINDOW = 48
X_ROWS = 440
LANES = 128
TILES = 14
COLS = TILES * LANES
ROWS = 12
BLOCK = ROWS * TILES
BF = jnp.bfloat16
F32 = jnp.float32
MESH = pl.DeviceIdType.MESH
FULL_SCALE = 32000.0
LOG_STEP = float(np.log(2.0) / 64.0)

LOW_TILE = 1
HIGH_TILE = 10


def split_np(table):
    high = table.astype(np.float32).astype(jnp.bfloat16)
    low = (table - high.astype(np.float64)).astype(np.float32).astype(jnp.bfloat16)
    return high, low


def twiddles():
    phase = (np.arange(G)[:, None] * np.arange(G)[None, :]) % G
    angle = phase * (2.0 * np.pi / G)
    cos_part, sine_part = np.cos(angle), np.sin(angle)
    freq = (6 * np.arange(NY)[None, :] + np.arange(6)[:, None]).reshape(-1)
    x_rows = np.concatenate([cos_part[freq], -sine_part[freq]], axis=0)
    both = np.concatenate([cos_part, sine_part], axis=1)
    return split_np(x_rows) + split_np(both)


def split(value):
    high = value.astype(BF)
    return high, (value - high.astype(F32)).astype(BF)


def level_code(largest):
    return jnp.clip(jnp.ceil(jnp.log(jnp.maximum(largest, 1e-30)) * (1.0 / LOG_STEP)), -8000.0, 8000.0)


def dot(a, b):
    return lax.dot_general(a, b, (((1,), (0,)), ((), ())), preferred_element_type=F32)


def dot_nt(a, b):
    return lax.dot_general(a, b, (((1,), (1,)), ((), ())), preferred_element_type=F32)


def row_iota(first, rows):
    return lax.broadcasted_iota(jnp.int32, (rows, CHUNK), 0) + first


def pick(rows, positions, weights):
    line = jnp.where(rows == positions[3], weights[3], 0.0)
    for s in (2, 1, 0):
        line = jnp.where(rows == positions[s], weights[s], line)
    return line


def sort_rows(keys):
    lane = lax.broadcasted_iota(jnp.int32, keys[0].shape, 1)
    keys = list(keys)
    size = 2
    while size <= LANES * len(keys):
        distance = size // 2
        while distance >= LANES:
            apart = distance // LANES
            for v in range(len(keys)):
                if not v & apart:
                    a, b = keys[v], keys[v + apart]
                    low, high = jnp.minimum(a, b), jnp.maximum(a, b)
                    up = not v & (size // LANES)
                    keys[v], keys[v + apart] = (low, high) if up else (high, low)
            distance //= 2
        while distance:
            lower = lax.bitwise_and(lane, distance) == 0
            for v, key in enumerate(keys):
                other = jnp.where(lower, pltpu.roll(key, LANES - distance, 1), pltpu.roll(key, distance, 1))
                low, high = jnp.minimum(key, other), jnp.maximum(key, other)
                if size < LANES:
                    keys[v] = jnp.where(lower == (lax.bitwise_and(lane, size) == 0), low, high)
                elif v & (size // LANES):
                    keys[v] = jnp.where(lower, high, low)
                else:
                    keys[v] = jnp.where(lower, low, high)
            distance //= 2
        size *= 2
    return keys


def spread_kernel(
    w_ref, idx_ref, q_ref, m_ref, fh_ref, fl_ref, msg_ref,
    acc_ref, xl_ref, yl_ref, qh_ref, ql_ref, modes_ref, rows_ref, raw_ref, raw_base_ref, wgt_ref, base_ref, key_ref, *bufs,
):
    groups = LANES // 8

    def unstack(block, carry):
        for k in range(8):
            row = 8 * block + k
            span = pl.ds(pl.multiple_of(row * LANES, LANES), LANES)
            for dim in range(3):
                raw_base_ref[dim, pl.ds(row, 1), :] = idx_ref[dim : dim + 1, span]
                for s in range(TAPS):
                    raw_ref[TAPS * dim + s, pl.ds(row, 1), :] = w_ref[dim, s : s + 1, span]
        return carry

    lax.fori_loop(0, groups, unstack, 0)
    lane = lax.broadcasted_iota(jnp.int32, (8, LANES), 1)
    keys = []
    for v in range(groups):
        rows = slice(8 * v, 8 * v + 8)
        keys.append((raw_base_ref[0, rows, :] * (LANES * groups) + (lane + LANES * v)).astype(F32))
        raw_base_ref[1, rows, :] = raw_base_ref[1, rows, :] * 256 + raw_base_ref[2, rows, :]
        charge = q_ref[rows, :] * m_ref[rows, :].astype(F32)
        for s in range(TAPS):
            raw_ref[s, rows, :] = raw_ref[s, rows, :] * charge
    for v, key in enumerate(sort_rows(keys)):
        key_ref[8 * v : 8 * v + 8, :] = key.astype(jnp.int32)

    def permute(v, carry):
        rows = pl.ds(pl.multiple_of(8 * v, 8), 8)
        key = key_ref[rows, :]
        base_ref[0, rows, :] = lax.shift_right_logical(key, 11)
        vector = lax.bitwise_and(lax.shift_right_logical(key, 7), groups - 1)
        source = lax.bitwise_and(key, LANES - 1)
        hits = [vector == k for k in range(groups)]

        def place(ref, field):
            value = jnp.take_along_axis(ref[field, 0:8, :], source, axis=1)
            for k in range(1, groups):
                value = jnp.where(hits[k], jnp.take_along_axis(ref[field, 8 * k : 8 * k + 8, :], source, axis=1), value)
            return value

        both = place(raw_base_ref, 1)
        base_ref[1, rows, :] = lax.shift_right_logical(both, 8)
        base_ref[2, rows, :] = lax.bitwise_and(both, 255)
        for field in range(3 * TAPS):
            wgt_ref[field, rows, :] = place(raw_ref, field)
        return carry

    lax.fori_loop(0, groups, permute, 0)

    def row_of(ref, field, step):
        pieces = [
            jnp.broadcast_to(ref[field, pl.ds(2 * step + k, 1), :], (16, LANES)) for k in range(2)
        ]
        return jnp.concatenate(pieces, axis=1)

    def taps(dim, step, first):
        base = row_of(base_ref, dim, step) - first
        return [base + s for s in range(TAPS)], [row_of(wgt_ref, TAPS * dim + s, step) for s in range(TAPS)]

    def x_line(step, first):
        pos_x, wgt_x = taps(0, step, first)
        for g in range(WINDOW // 16):
            xl_ref[16 * g : 16 * g + 16, :] = pick(row_iota(16 * g, 16), pos_x, wgt_x)

    def build_head(step, ah, al, zh, zl):
        bases = base_ref[0, pl.ds(2 * step, 2), :]
        first = jnp.min(bases) // 8 * 8
        windows = (jnp.max(bases) + 3 - first) // WINDOW + 1
        x_line(step, first)
        pos_y, wgt_y = taps(1, step, 0)
        yl_ref[...] = pick(row_iota(0, 16), pos_y, wgt_y)
        pos_z, wgt_z = taps(2, step, 0)
        for g in range(LEN_Z // 16 + 1):
            rows = slice(16 * g, 16 * g + 16)
            zh[rows, :], zl[rows, :] = split(pick(row_iota(16 * g, 16), pos_z, wgt_z))
        return first, windows

    def build_group(step, group, ah, al):
        for y in range(3 * group, 3 * group + 3):
            line = jnp.broadcast_to(yl_ref[y : y + 1, :], (16, CHUNK))
            for g in range(WINDOW // 16):
                rows = slice(WINDOW * y + 16 * g, WINDOW * y + 16 * g + 16)
                ah[rows, :], al[rows, :] = split(xl_ref[16 * g : 16 * g + 16, :] * line)

    def accumulate(first, group, ah, al, zh, zl):
        span = pl.ds(pl.multiple_of(first, 8), WINDOW)
        rows = slice(3 * WINDOW * group, 3 * WINDOW * (group + 1))
        part = dot_nt(ah[rows, :], zh[...]) + dot_nt(al[rows, :], zh[...]) + dot_nt(ah[rows, :], zl[...])
        for k in range(3):
            acc_ref[3 * group + k, span, :] += part[WINDOW * k : WINDOW * k + WINDOW]

    def stage(step, first, current, following):
        ahead = build_head(step, *following)
        for group in range(3):
            accumulate(first, group, *current)
            build_group(step, group, *following[:2])
        return ahead

    def remaining(step, first, windows, ah, al, zh, zl):
        def window(k, carry):
            x_line(step, first + WINDOW * k)
            pos_y, wgt_y = taps(1, step, 0)
            yl_ref[...] = pick(row_iota(0, 16), pos_y, wgt_y)
            for group in range(3):
                build_group(step, group, ah, al)
                accumulate(first + WINDOW * k, group, ah, al, zh, zl)
            return carry

        lax.fori_loop(1, windows, window, 0)

    one, two = bufs[:4], bufs[4:]
    acc_ref[...] = jnp.zeros_like(acc_ref)
    for buf in (one[2], one[3], two[2], two[3]):
        buf[...] = jnp.zeros_like(buf)
    chunks = LANES * LANES // CHUNK

    def body(pair, carry):
        first, windows = carry
        ahead = stage(2 * pair + 1, first, one, two)
        remaining(2 * pair, first, windows, *one)
        last = stage(jnp.minimum(2 * pair + 2, chunks - 1), ahead[0], two, one)
        remaining(2 * pair + 1, *ahead, *two)
        return last

    start = build_head(0, *one)
    for group in range(3):
        build_group(0, group, *one[:2])
    lax.fori_loop(0, chunks // 2, body, start)

    lane = lax.broadcasted_iota(jnp.int32, (G, LANES), 1)

    def put(t, value):
        cols = slice(LANES * t, LANES * t + LANES)
        qh_ref[:, cols], ql_ref[:, cols] = split(value)

    for y in range(EXT_Y):
        acc_ref[y, 0:8, :] += acc_ref[y, G : G + 8, :]
        put(LOW_TILE + y, acc_ref[y, :G, :LANES])
        high = acc_ref[y, :G, LANES:]
        ghost = jnp.where(lane < 64, 0.0, high)
        ghosts = ghost if y == 0 else ghosts + pltpu.roll(ghost, 4 * y, 1)
        if y == 8:
            put(0, jnp.where(lane < 64, high, ghosts))
        elif y % 2:
            put(HIGH_TILE + y // 2, jnp.where(lane < 64, even, pltpu.roll(high, 64, 1)))
        else:
            even = high
    for t in range(TILES // 2):
        cols = slice(256 * t, 256 * t + 256)
        part = dot(fh_ref[...], qh_ref[:, cols]) + dot(fl_ref[...], qh_ref[:, cols]) + dot(fh_ref[...], ql_ref[:, cols])
        modes_ref[:, cols] = part
        size = jnp.maximum(jnp.abs(part[:, :LANES]), jnp.abs(part[:, LANES:]))
        largest = size if t == 0 else jnp.maximum(largest, size)
    code = level_code(jnp.max(largest, axis=1, keepdims=True))
    inverse = jnp.exp(code * (-LOG_STEP)) * FULL_SCALE
    lane = lax.broadcasted_iota(jnp.int32, (ROWS * NY, LANES), 1)
    for t in range(TILES):
        value = modes_ref[:, LANES * t : LANES * t + LANES] * inverse
        if t == 0:
            value = jnp.where(lane == LANES - 1, code, value)
        for r in range(ROWS):
            rows_ref[pl.ds(t * ROWS + r, NY, stride=BLOCK), :] = value[NY * r : NY * r + NY, :]

    def pack(peer, carry):
        span = pl.ds(pl.multiple_of(peer * BLOCK, 8), BLOCK)
        value = lax.round(rows_ref[span, :], lax.RoundingMethod.TO_NEAREST_EVEN)
        msg_ref[peer] = value.astype(jnp.int32).astype(jnp.int16)
        return carry

    lax.fori_loop(0, NY, pack, 0)


def spread(w, idx, charge, mask, fh, fl):
    return pl.pallas_call(
        spread_kernel,
        out_shape=jax.ShapeDtypeStruct((NY, BLOCK, LANES), jnp.int16),
        in_specs=[pl.BlockSpec(memory_space=pltpu.VMEM)] * 6,
        out_specs=pl.BlockSpec(memory_space=pltpu.VMEM),
        scratch_shapes=[
            pltpu.VMEM((EXT_Y, X_ROWS, 2 * LANES), F32),
            pltpu.VMEM((WINDOW, CHUNK), F32),
            pltpu.VMEM((16, CHUNK), F32),
            pltpu.VMEM((G, COLS), BF),
            pltpu.VMEM((G, COLS), BF),
            pltpu.VMEM((ROWS * NY, COLS), F32),
            pltpu.VMEM((NY * BLOCK, LANES), F32),
        ]
        + [
            pltpu.VMEM((3 * TAPS, LANES, LANES), F32),
            pltpu.VMEM((3, LANES, LANES), jnp.int32),
            pltpu.VMEM((3 * TAPS, LANES, LANES), F32),
            pltpu.VMEM((3, LANES, LANES), jnp.int32),
            pltpu.VMEM((LANES, LANES), jnp.int32),
        ]
        + [
            pltpu.VMEM((EXT_Y * WINDOW, CHUNK), BF),
            pltpu.VMEM((EXT_Y * WINDOW, CHUNK), BF),
            pltpu.VMEM((2 * LANES, CHUNK), BF),
            pltpu.VMEM((2 * LANES, CHUNK), BF),
        ]
        * 2,
        compiler_params=pltpu.CompilerParams(vmem_limit_bytes=60 * 1024 * 1024),
        name="spread",
    )(w, idx, charge, mask, fh, fl)


def exchange_kernel(msg_ref, recv_ref, ghost_ref, send_sem, recv_sem, ghost_send_sem, ghost_recv_sem):
    me, half = lax.axis_index("ydom"), lax.axis_index("zdom")
    barrier = pltpu.get_barrier_semaphore()

    def greet(peer, carry):
        for side in range(2):
            pl.semaphore_signal(barrier, inc=1, device_id={"ydom": peer, "zdom": side}, device_id_type=MESH)
        return carry

    lax.fori_loop(0, NY, greet, 0)
    pl.semaphore_wait(barrier, 2 * NY)

    def peer_of(step):
        shift = lax.rem(step * 23, NY)
        x = lax.rem(me + shift, 4)
        y = lax.rem(me // 4 + shift // 4, 4)
        z = lax.rem(me // 16 + shift // 16, 4)
        return x + 4 * y + 16 * z

    def send_ghost(step, carry):
        peer = peer_of(step)
        pltpu.make_async_remote_copy(
            src_ref=msg_ref.at[peer, pl.ds(0, 16)],
            dst_ref=ghost_ref.at[me],
            send_sem=ghost_send_sem,
            recv_sem=ghost_recv_sem,
            device_id={"ydom": peer, "zdom": 1 - half},
            device_id_type=MESH,
        ).start()
        return carry

    def send(step, carry):
        peer = peer_of(step)
        pltpu.make_async_remote_copy(
            src_ref=msg_ref.at[peer],
            dst_ref=recv_ref.at[me],
            send_sem=send_sem,
            recv_sem=recv_sem,
            device_id={"ydom": peer},
            device_id_type=MESH,
        ).start()
        return carry

    lax.fori_loop(1, NY, send, 0)
    lax.fori_loop(0, NY, send_ghost, 0)
    recv_ref[me] = msg_ref[me]
    others = pl.ds(0, NY - 1)
    pltpu.make_async_copy(recv_ref.at[others], recv_ref.at[others], recv_sem).wait()
    pltpu.make_async_copy(ghost_ref, ghost_ref, ghost_recv_sem).wait()
    pltpu.make_async_copy(recv_ref.at[others], recv_ref.at[others], send_sem).wait()
    pltpu.make_async_copy(ghost_ref, ghost_ref, ghost_send_sem).wait()


def exchange(msg):
    return pl.pallas_call(
        exchange_kernel,
        out_shape=(
            jax.ShapeDtypeStruct((NY, BLOCK, LANES), jnp.int16),
            jax.ShapeDtypeStruct((NY, 16, LANES), jnp.int16),
        ),
        in_specs=[pl.BlockSpec(memory_space=pltpu.VMEM)],
        out_specs=(pl.BlockSpec(memory_space=pltpu.VMEM),) * 2,
        scratch_shapes=[pltpu.SemaphoreType.DMA] * 4,
        compiler_params=pltpu.CompilerParams(
            vmem_limit_bytes=16 * 1024 * 1024, collective_id=0, has_side_effects=True
        ),
        name="exchange",
    )(msg)


def y_kernel(
    recv16_ref, ghost16_ref, ch_ref, cl_ref, own_ref, other_ref,
    recv_ref, ghost_ref, x_ref, rh_ref, rl_ref, away_ref, send_sems, recv_sems,
):
    side = lax.axis_index("zdom")
    barrier = pltpu.get_barrier_semaphore()
    pl.semaphore_signal(barrier, inc=1, device_id={"zdom": 1 - side}, device_id_type=MESH)

    def unpack(peer, carry):
        span = pl.ds(pl.multiple_of(peer * BLOCK, 8), BLOCK)
        recv_ref[span, :] = recv16_ref[peer].astype(jnp.int32).astype(F32)
        span = pl.ds(pl.multiple_of(peer * 16, 8), 16)
        ghost_ref[span, :] = ghost16_ref[peer].astype(jnp.int32).astype(F32)
        return carry

    lax.fori_loop(0, NY, unpack, 0)
    copies = []
    lane = lax.broadcasted_iota(jnp.int32, (NY, LANES), 1)

    def raw(t, row):
        return recv_ref[pl.ds(t * ROWS + row, NY, stride=BLOCK), :]

    def level(coded):
        return jnp.broadcast_to(jnp.exp(coded[:, LANES - 1 :] * LOG_STEP) * (1.0 / FULL_SCALE), (NY, LANES))

    def before(value):
        return pltpu.roll(value, 1, 0)

    def half_turn(value):
        return pltpu.roll(value, 64, 1)

    for pair in range(3):
        for part in range(2):
            high_tiles = []
            for odd in range(2):
                row = 6 * part + 2 * pair + odd
                edge = raw(0, row)
                scale = level(edge)
                edge = edge * scale
                ghost = ghost_ref[pl.ds(row, NY, stride=16), :]
                ghost = ghost * level(ghost)

                def tile(t, row):
                    return raw(t, row) * scale

                def low(y):
                    moved = pltpu.roll(ghost, LANES - 64 - 4 * y, 1)
                    return tile(LOW_TILE + y, row) + jnp.where(lane < 3, moved, 0.0)

                for y in range(LEN_Y):
                    value = low(y)
                    if y < 3:
                        value = value + before(low(y + 6))
                    x_ref[pl.ds(G * odd + y, NY, stride=LEN_Y), :] = value
                tiles = [tile(HIGH_TILE + k, row) for k in range(3)]
                tiles[0] = tiles[0] + before(tile(HIGH_TILE + 3, row))
                tiles[1] = tiles[1] + jnp.where(lane < 64, before(edge), 0.0)
                high_tiles.append(tiles)
            for k in range(3):
                even, odd = high_tiles[0][k], high_tiles[1][k]
                x_ref[pl.ds(2 * G + 2 * k, NY, stride=LEN_Y), :] = jnp.where(lane < 64, even, half_turn(odd))
                x_ref[pl.ds(2 * G + 2 * k + 1, NY, stride=LEN_Y), :] = jnp.where(lane < 64, half_turn(even), odd)
            for k in range(3):
                high, low_part = split(x_ref[G * k : G * k + G, :])
                own = slice(G * part + LANES * k, G * part + LANES * k + LANES)
                rh_ref[0:G, own] = high
                rl_ref[0:G, own] = low_part
                swapped = slice(G * (1 - part) + LANES * k, G * (1 - part) + LANES * k + LANES)
                rh_ref[G : 2 * G, swapped] = high if part else -high
                rl_ref[G : 2 * G, swapped] = low_part if part else -low_part
        for t in range(3):
            cols = slice(256 * t, 256 * t + 256)
            part = (
                dot(ch_ref[...], rh_ref[:, cols]) + dot(cl_ref[...], rh_ref[:, cols]) + dot(ch_ref[...], rl_ref[:, cols])
            )
            upper, lower = part[:LEN_Z], part[LEN_Z:]
            own_ref[pair, :, cols] = jnp.where(side == 0, upper, lower)
            away_ref[pair, :, cols] = jnp.where(side == 0, lower, upper)
        if pair == 0:
            pl.semaphore_wait(barrier, 1)
        copies.append(
            pltpu.make_async_remote_copy(
                src_ref=away_ref.at[pair],
                dst_ref=other_ref.at[pair],
                send_sem=send_sems.at[pair],
                recv_sem=recv_sems.at[pair],
                device_id={"zdom": 1 - side},
                device_id_type=MESH,
            )
        )
        copies[-1].start()
    for copy in copies:
        copy.wait()


def y_transform(recv, ghost, ch, cl):
    half = jax.ShapeDtypeStruct((3, LEN_Z, 2 * G), F32)
    return pl.pallas_call(
        y_kernel,
        out_shape=(half, half),
        in_specs=[pl.BlockSpec(memory_space=pltpu.VMEM)] * 4,
        out_specs=(pl.BlockSpec(memory_space=pltpu.VMEM),) * 2,
        scratch_shapes=[
            pltpu.VMEM((NY * BLOCK, LANES), F32),
            pltpu.VMEM((NY * 16, LANES), F32),
            pltpu.VMEM((3 * G, LANES), F32),
            pltpu.VMEM((2 * G, 2 * G), BF),
            pltpu.VMEM((2 * G, 2 * G), BF),
            pltpu.VMEM((3, LEN_Z, 2 * G), F32),
            pltpu.SemaphoreType.DMA((3,)),
            pltpu.SemaphoreType.DMA((3,)),
        ],
        compiler_params=pltpu.CompilerParams(
            vmem_limit_bytes=40 * 1024 * 1024, collective_id=1, has_side_effects=True
        ),
        name="y_transform",
    )(recv, ghost, ch, cl)


def z_kernel(
    own_ref, other_ref, ch_ref, cl_ref, bc_ref, out_ref, sum_ref,
    rh_ref, rl_ref, lh_ref, ll_ref, part_ref, parts_ref, pair_ref, sems,
):
    me, side = lax.axis_index("ydom"), lax.axis_index("zdom")
    barrier = pltpu.get_barrier_semaphore()

    def greet(step, carry):
        pl.semaphore_signal(barrier, inc=1, device_id={"ydom": lax.rem(me + step, NY)}, device_id_type=MESH)
        return carry

    lax.fori_loop(1, NY, greet, 0)
    pl.semaphore_signal(barrier, inc=1, device_id={"zdom": 1 - side}, device_id_type=MESH)
    lane = lax.broadcasted_iota(jnp.int32, (LEN_Z, LANES), 1)
    for src, dst in ((ch_ref, rh_ref), (cl_ref, rl_ref)):

        def place(first, rows, half, z, part):
            span = pl.ds(pl.multiple_of(LEN_Z * (side if half == 0 else 1 - side) + z, 64), rows)
            cos_part = src[span, 0:G]
            sine_part = src[span, G : 2 * G]
            dst[first : first + rows, 0:G] = sine_part if part else cos_part
            dst[first : first + rows, G : 2 * G] = cos_part if part else -sine_part

        for half in range(2):
            for part in range(2):
                place(LANES * (2 * half + part), LANES, half, 0, part)
                place(512 + LANES * half + 64 * part, 64, half, LANES, part)
    total = jnp.zeros((8, G), F32)
    for pair in range(3):
        for odd in range(2):
            rows = slice(LEN_Z * odd, LEN_Z * odd + LEN_Z)

            def put(col, value):
                high, low = split(value)
                lh_ref[rows, col : col + LANES] = high
                ll_ref[rows, col : col + LANES] = low

            for half, in_ref in enumerate((own_ref, other_ref)):
                highs = []
                for part in range(2):
                    first = G * part + LANES * odd
                    put(LANES * (2 * half + part), in_ref[pair, :, first : first + LANES])
                    highs.append(in_ref[pair, :, G * part + 256 : G * part + 384])
                if odd:
                    merged = jnp.where(lane < 64, pltpu.roll(highs[0], 64, 1), highs[1])
                else:
                    merged = jnp.where(lane < 64, highs[0], pltpu.roll(highs[1], 64, 1))
                put(512 + LANES * half, merged)
        mode = (
            dot(lh_ref[...], rh_ref[...]) + dot(ll_ref[...], rh_ref[...]) + dot(lh_ref[...], rl_ref[...])
        )
        for odd in range(2):
            real = mode[LEN_Z * odd : LEN_Z * odd + LEN_Z, 0:G]
            imag = mode[LEN_Z * odd : LEN_Z * odd + LEN_Z, G : 2 * G]
            value = 0.5 * bc_ref[2 * pair + odd] * (real * real + imag * imag)
            out_ref[2 * pair + odd] = value
            total = total + jnp.sum(value.reshape(LEN_Z // 8, 8, G), axis=0)
    lanes = total[:, :LANES] + total[:, LANES : 2 * LANES] + total[:, 2 * LANES :]
    part_ref[...] = jnp.sum(lanes, axis=0, keepdims=True)
    pl.semaphore_wait(barrier, NY)

    def send(step, carry):
        pltpu.make_async_remote_copy(
            src_ref=part_ref,
            dst_ref=parts_ref.at[me],
            send_sem=sems.at[0],
            recv_sem=sems.at[1],
            device_id={"ydom": lax.rem(me + step, NY)},
            device_id_type=MESH,
        ).start()
        return carry

    lax.fori_loop(1, NY, send, 0)
    parts_ref[me] = part_ref[...]
    others = pl.ds(0, NY - 1)
    pltpu.make_async_copy(parts_ref.at[others], parts_ref.at[others], sems.at[1]).wait()
    pltpu.make_async_copy(parts_ref.at[others], parts_ref.at[others], sems.at[0]).wait()
    pair_ref[0] = jnp.sum(parts_ref[...], axis=0)
    copy = pltpu.make_async_remote_copy(
        src_ref=pair_ref.at[0],
        dst_ref=pair_ref.at[1],
        send_sem=sems.at[2],
        recv_sem=sems.at[3],
        device_id={"zdom": 1 - side},
        device_id_type=MESH,
    )
    copy.start()
    copy.wait()
    energy = jnp.sum(pair_ref[0] + pair_ref[1], axis=1, keepdims=True) * (1.0 / (G * G * G))
    sum_ref[...] = jnp.broadcast_to(energy, (1, LANES))


def z_transform(own, other, ch, cl, influence):
    return pl.pallas_call(
        z_kernel,
        out_shape=(jax.ShapeDtypeStruct((6, LEN_Z, G), F32), jax.ShapeDtypeStruct((1, LANES), F32)),
        in_specs=[pl.BlockSpec(memory_space=pltpu.VMEM)] * 5,
        out_specs=(pl.BlockSpec(memory_space=pltpu.VMEM),) * 2,
        scratch_shapes=[pltpu.VMEM((2 * G, 2 * G), BF)] * 2
        + [pltpu.VMEM((G, 2 * G), BF)] * 2
        + [
            pltpu.VMEM((1, LANES), F32),
            pltpu.VMEM((NY, 1, LANES), F32),
            pltpu.VMEM((2, 1, LANES), F32),
            pltpu.SemaphoreType.DMA((4,)),
        ],
        compiler_params=pltpu.CompilerParams(
            vmem_limit_bytes=40 * 1024 * 1024, collective_id=2, has_side_effects=True
        ),
        name="z_transform",
    )(own, other, ch, cl, influence)


def solution(mesh):
    slots = ('sys', 'ydom', 'zdom')
    mode_spec = P(('sys', 'ydom'), 'zdom', None)
    tables = twiddles()

    def local_energy(charge, real_mask, grid_idx, spline_w, influence):
        fh, fl, ch, cl = [jnp.asarray(table) for table in tables]
        square = (LANES, LANES)
        w = jnp.transpose(spline_w, (1, 2, 0))
        idx = jnp.transpose(grid_idx, (1, 0))
        msg = spread(w, idx, charge.reshape(square), real_mask.reshape(square), fh, fl)
        recv, ghost = exchange(msg)
        own, other = y_transform(recv, ghost, ch, cl)
        mode_energy, energy = z_transform(own, other, ch, cl, influence)
        return mode_energy, energy[0, :1]

    return jax.shard_map(local_energy, mesh=mesh, in_specs=(P(slots), P(slots), P(slots, None), P(slots, None, None), mode_spec), out_specs=(mode_spec, P('sys')), check_vma=False)
```
